32 devices in a mesh: section: 2 (over core), ctx: 4 (over y, x), fsdp: 4 (over z).
Axes of the slice: x: 2, y: 2, z: 4, core: 2. Of those that a mesh axis runs over, the one named last changes fastest.
Arguments:
- tokens: bfloat16 [2, 4, 768, 640], P(None, 'fsdp', 'ctx'), may hold values from -6 to 6
- cotangent: bfloat16 [2, 4, 768, 640], P(None, 'fsdp', 'ctx'), may hold values from -6 to 6
- block_map: int32 [4, 2], replicated, may hold values from 0 to 7, as said below
- order: int32 [4, 2], P('fsdp'), may hold values from 0 to 1, each once within a row
- w_query: bfloat16 [2, 640, 1024], P('section', ('ctx', 'fsdp')), may hold values from -0.25 to 0.25
- w_key: bfloat16 [2, 640, 256], P('section', ('ctx', 'fsdp')), may hold values from -0.25 to 0.25
- w_value: bfloat16 [2, 640, 256], P('section', ('ctx', 'fsdp')), may hold values from -0.25 to 0.25
- w_out: bfloat16 [2, 1024, 640], P('section', ('ctx', 'fsdp')), may hold values from -2.5 to 2.5
- w_gate: bfloat16 [2, 640, 2048], P('section', ('ctx', 'fsdp')), may hold values from -0.25 to 0.25
- w_up: bfloat16 [2, 640, 2048], P('section', ('ctx', 'fsdp')), may hold values from -0.25 to 0.25
- w_down: bfloat16 [2, 2048, 640], P('section', ('ctx', 'fsdp')), may hold values from -0.125 to 0.125
- g_attn: bfloat16 [2, 640], P('section', ('ctx', 'fsdp')), may hold values from 0.099609375 to 1.8984375
- g_ffn: bfloat16 [2, 640], P('section', ('ctx', 'fsdp')), may hold values from 0.099609375 to 1.8984375
- g_query: bfloat16 [2, 256], P('section', ('ctx', 'fsdp')), may hold values from 0.099609375 to 1.8984375
- g_key: bfloat16 [2, 256], P('section', ('ctx', 'fsdp')), may hold values from 0.099609375 to 1.8984375
Outputs:
- section_out: bfloat16 [2, 2, 4, 768, 640], P('section', None, 'fsdp', 'ctx')
- in_grad: bfloat16 [2, 2, 4, 768, 640], P('section', None, 'fsdp', 'ctx')
- grad_query: float32 [2, 640, 1024], P('section', ('ctx', 'fsdp'))
- grad_key: float32 [2, 640, 256], P('section', ('ctx', 'fsdp'))
- grad_value: float32 [2, 640, 256], P('section', ('ctx', 'fsdp'))
- grad_out: float32 [2, 1024, 640], P('section', ('ctx', 'fsdp'))
- grad_gate: float32 [2, 640, 2048], P('section', ('ctx', 'fsdp'))
- grad_up: float32 [2, 640, 2048], P('section', ('ctx', 'fsdp'))
- grad_down: float32 [2, 2048, 640], P('section', ('ctx', 'fsdp'))
- grad_attn_gain: float32 [2, 640], P('section', ('ctx', 'fsdp'))
- grad_ffn_gain: float32 [2, 640], P('section', ('ctx', 'fsdp'))
- grad_query_gain: float32 [2, 256], P('section', ('ctx', 'fsdp'))
- grad_key_gain: float32 [2, 256], P('section', ('ctx', 'fsdp'))
The draws below stay inside these ranges and needn't reach their ends.
Inputs may be any that keep to these rules, and one draw needn't show every extreme that they name: `block_map`: row c lists the blocks, of 96 positions each, stored at ctx index c in that order; every block 0 to 7 is listed exactly once. `order`: each row is a permutation of the micro-batches.
All inputs are finite; a program needn't handle non-finite values.
Results may differ from the reference program's by a relative error of at most 0.025.
Values may be sent and summed in bfloat16 or wider, within the bound.
A program may use at most 256 MiB of HBM per device.

```python
import jax
import jax.numpy as jnp
from jax import lax

D = 640
QH = 4
HD = 256
FF = 2048
BLK = 96
MB = 2
NBLK = 8
SEQ = 768
NSEQ = 4


def draw_block_map(key, part):
    shuffled = jax.random.permutation(key, NBLK)
    return shuffled.reshape(NBLK // 2, 2).astype(jnp.int32)


def steps_of(rng, extent, split, low, high):
    def one(axis_at, shards_of):
        steps = jax.random.uniform(jax.random.fold_in(jax.random.fold_in(rng, 6), axis_at), (shards_of,), jnp.float32, low / len(split), high / len(split))
        return jnp.repeat(jnp.exp(steps), extent[axis_at] // shards_of).reshape((-1,) + (1,) * (len(extent) - axis_at - 1))

    loudness = one(*split[0])
    for cut in split[1:]:
        loudness = loudness * one(*cut)
    return loudness


def scatter_about(key, dims, deviation, reach, pieces=(), kind=jnp.bfloat16):
    values = deviation * jax.random.normal(key, dims, jnp.float32)
    if pieces:
        values = values * steps_of(key, dims, pieces, -0.22, 0.18)
    return jnp.clip(values, -reach, reach).astype(kind)


def setup_inputs(seed: int = 0) -> dict:
    splits = jax.random.split(jax.random.key(seed), 16)
    tokens = scatter_about(splits[0], (MB, NSEQ, SEQ, D), 1.0, 6.0, ((1, 4), (2, 4)))
    cotangent = scatter_about(splits[1], (MB, NSEQ, SEQ, D), 1.0, 6.0, ((1, 4), (2, 4)))
    block_map = draw_block_map(jax.random.fold_in(splits[15], 71), 0)
    order = jax.vmap(lambda own: jax.random.permutation(own, MB))(jax.random.split(splits[3], NSEQ)).reshape((NSEQ, MB)).astype(jnp.int32)
    w_query = scatter_about(splits[4], (2, D, QH * HD), D ** -0.5, 0.25, ((0, 2), (1, 16)))
    w_key = scatter_about(splits[5], (2, D, HD), D ** -0.5, 0.25, ((0, 2), (1, 16)))
    w_value = scatter_about(splits[6], (2, D, HD), D ** -0.5, 0.25, ((0, 2), (1, 16)))
    w_out = scatter_about(splits[7], (2, QH * HD, D), (max(1, 4 * QH * HD // SEQ)) ** -0.5, 2.5, ((0, 2), (1, 16)))
    w_gate = scatter_about(splits[8], (2, D, FF), D ** -0.5, 0.25, ((0, 2), (1, 16)))
    w_up = scatter_about(splits[9], (2, D, FF), D ** -0.5, 0.25, ((0, 2), (1, 16)))
    w_down = scatter_about(splits[10], (2, FF, D), FF ** -0.5, 0.125, ((0, 2), (1, 16)))
    g_attn = jnp.clip(1.0 + 0.18 * jax.random.normal(splits[11], (2, D), jnp.float32), 0.099609375, 1.8984375).astype(jnp.bfloat16)
    g_ffn = jnp.clip(1.0 + 0.18 * jax.random.normal(splits[12], (2, D), jnp.float32), 0.099609375, 1.8984375).astype(jnp.bfloat16)
    g_query = jnp.clip(1.0 + 0.18 * jax.random.normal(splits[13], (2, HD), jnp.float32), 0.099609375, 1.8984375).astype(jnp.bfloat16)
    g_key = jnp.clip(1.0 + 0.18 * jax.random.normal(splits[14], (2, HD), jnp.float32), 0.099609375, 1.8984375).astype(jnp.bfloat16)
    return {"tokens": tokens, "cotangent": cotangent, "block_map": block_map, "order": order, "w_query": w_query, "w_key": w_key, "w_value": w_value, "w_out": w_out, "w_gate": w_gate, "w_up": w_up, "w_down": w_down, "g_attn": g_attn, "g_ffn": g_ffn, "g_query": g_query, "g_key": g_key}


EPS = 1e-06

def rms_scale(values, gain):
    mean_square = lax.optimization_barrier(jnp.mean(values * values, axis=-1, keepdims=True))
    return values * lax.rsqrt(mean_square + EPS) * gain

def norm_pull(values, gain, upstream):
    _, pull = jax.vjp(rms_scale, values, gain)
    return pull(upstream)

def glu_act(gate_part, up_part):
    return jax.nn.gelu(gate_part, approximate=True) * up_part

def fdot(left, right):
    return jnp.dot(left, right, preferred_element_type=jnp.float32)

def fsum(form, left, right):
    return jnp.einsum(form, left.astype(jnp.float32), right.astype(jnp.float32))

def masked_scores(query_n, key_n, positions):
    head_dim = query_n.shape[-1]
    scores = fsum('rhd,sd->hrs', query_n, key_n) * head_dim ** (-0.5)
    allowed = positions[None, None, :] <= positions[None, :, None]
    return jnp.where(allowed, scores, -jnp.inf)

def layer_forward(inputs, params, positions):
    w_query, w_key, w_value, w_out, w_gate, w_up, w_down, g_attn, g_ffn, g_query, g_key = params
    head_dim = g_query.shape[0]
    count = inputs.shape[0]
    resid = inputs.astype(jnp.float32)
    normed = rms_scale(resid, g_attn.astype(jnp.float32)).astype(jnp.bfloat16)
    query = fdot(normed, w_query)
    key_raw = fdot(normed, w_key)
    value = fdot(normed, w_value).astype(jnp.bfloat16)
    query_n = rms_scale(query.reshape(count, -1, head_dim), g_query.astype(jnp.float32)).astype(jnp.bfloat16)
    key_n = rms_scale(key_raw, g_key.astype(jnp.float32)).astype(jnp.bfloat16)
    scores = masked_scores(query_n, key_n, positions)
    top = lax.optimization_barrier(jnp.max(scores, axis=-1, keepdims=True))
    lse = top + jnp.log(lax.optimization_barrier(jnp.sum(jnp.exp(scores - top), axis=-1, keepdims=True)))
    probs = jnp.exp(scores - lse).astype(jnp.bfloat16)
    mixed = fsum('hrs,sd->rhd', probs, value).reshape(count, -1).astype(jnp.bfloat16)
    middle = resid + fdot(mixed, w_out)
    ffn_in = rms_scale(middle, g_ffn.astype(jnp.float32)).astype(jnp.bfloat16)
    hidden = glu_act(fdot(ffn_in, w_gate), fdot(ffn_in, w_up)).astype(jnp.bfloat16)
    result = middle + fdot(hidden, w_down)
    return (result.astype(jnp.bfloat16), (inputs, query, key_raw, key_n, value, lse, mixed, middle))

def layer_backward(saved, upstream, params, positions):
    w_query, w_key, w_value, w_out, w_gate, w_up, w_down, g_attn, g_ffn, g_query, g_key = params
    inputs, query, key_raw, key_n, value, lse, mixed, middle = saved
    head_dim = g_query.shape[0]
    count = inputs.shape[0]
    gain_a = g_attn.astype(jnp.float32)
    gain_f = g_ffn.astype(jnp.float32)
    gain_q = g_query.astype(jnp.float32)
    gain_k = g_key.astype(jnp.float32)
    resid = inputs.astype(jnp.float32)
    ffn_in = rms_scale(middle, gain_f).astype(jnp.bfloat16)
    gate_part = fdot(ffn_in, w_gate)
    up_part = fdot(ffn_in, w_up)
    hidden = glu_act(gate_part, up_part).astype(jnp.bfloat16)
    top_b = upstream.astype(jnp.bfloat16)
    grad_down = fsum('rf,rd->fd', hidden, top_b)
    dhidden = fsum('rd,fd->rf', top_b, w_down)
    _, pull = jax.vjp(glu_act, gate_part, up_part)
    dgate, dup = pull(dhidden)
    dgate_b = dgate.astype(jnp.bfloat16)
    dup_b = dup.astype(jnp.bfloat16)
    grad_gate = fsum('rd,rf->df', ffn_in, dgate_b)
    grad_up = fsum('rd,rf->df', ffn_in, dup_b)
    dffn = fsum('rf,df->rd', dgate_b, w_gate) + fsum('rf,df->rd', dup_b, w_up)
    dmid_norm, grad_gf = norm_pull(middle, gain_f, dffn)
    dmiddle = upstream + dmid_norm
    dmid_b = dmiddle.astype(jnp.bfloat16)
    grad_out = fsum('rk,rd->kd', mixed, dmid_b)
    dmixed = fsum('rd,kd->rk', dmid_b, w_out).astype(jnp.bfloat16)
    query_heads = query.reshape(count, -1, head_dim)
    query_n = rms_scale(query_heads, gain_q).astype(jnp.bfloat16)
    scores = masked_scores(query_n, key_n, positions)
    probs = jnp.exp(scores - lse)
    dout = dmixed.reshape(count, -1, head_dim)
    dvalue = fsum('hrs,rhd->sd', probs.astype(jnp.bfloat16), dout)
    dprobs = fsum('rhd,sd->hrs', dout, value)
    inner = lax.optimization_barrier(jnp.sum(probs * dprobs, axis=-1, keepdims=True))
    dscore = (probs * (dprobs - inner) * head_dim ** (-0.5)).astype(jnp.bfloat16)
    dquery_n = fsum('hrs,sd->rhd', dscore, key_n)
    dkey_n = fsum('hrs,rhd->sd', dscore, query_n)
    dquery, grad_gq = norm_pull(query_heads, gain_q, dquery_n)
    dkey, grad_gk = norm_pull(key_raw, gain_k, dkey_n)
    dq_b = dquery.reshape(count, -1).astype(jnp.bfloat16)
    dk_b = dkey.astype(jnp.bfloat16)
    dv_b = dvalue.astype(jnp.bfloat16)
    normed = rms_scale(resid, gain_a).astype(jnp.bfloat16)
    grad_q = fsum('rd,rk->dk', normed, dq_b)
    grad_k = fsum('rd,rk->dk', normed, dk_b)
    grad_v = fsum('rd,rk->dk', normed, dv_b)
    dnormed = fsum('rk,dk->rd', dq_b, w_query) + fsum('rk,dk->rd', dk_b, w_key) + fsum('rk,dk->rd', dv_b, w_value)
    dres_norm, grad_ga = norm_pull(resid, gain_a, dnormed)
    dinput = dmiddle + dres_norm
    grads = (grad_q, grad_k, grad_v, grad_out, grad_gate, grad_up, grad_down, grad_ga, grad_gf, grad_gq, grad_gk)
    return (dinput.astype(jnp.bfloat16), grads)

def reference(tokens, cotangent, block_map, order, w_query, w_key, w_value, w_out, w_gate, w_up, w_down, g_attn, g_ffn, g_query, g_key):
    micro = tokens.shape[0]
    seqs = tokens.shape[1]
    starts = block_map.reshape(-1).astype(jnp.int32) * BLK
    positions = (starts[:, None] + jnp.arange(BLK, dtype=jnp.int32)[None, :]).reshape(-1)
    weights = (w_query, w_key, w_value, w_out, w_gate, w_up, w_down, g_attn, g_ffn, g_query, g_key)
    section_params = [tuple((w[s] for w in weights)) for s in range(2)]
    totals = [[jnp.zeros(w.shape[1:], jnp.float32) for w in weights] for s in range(2)]
    outs_first = []
    outs_second = []
    back_first = []
    back_second = []
    for slot in range(micro):
        row_a, row_b, row_c, row_d = ([], [], [], [])
        for seq in range(seqs):
            chosen = tokens[order[seq, slot], seq]
            first, saved_a = layer_forward(chosen, section_params[0], positions)
            second, saved_b = layer_forward(first, section_params[1], positions)
            back_b, grads_b = layer_backward(saved_b, cotangent[slot, seq].astype(jnp.float32), section_params[1], positions)
            back_a, grads_a = layer_backward(saved_a, back_b.astype(jnp.float32), section_params[0], positions)
            totals[0] = [acc + g for acc, g in zip(totals[0], grads_a)]
            totals[1] = [acc + g for acc, g in zip(totals[1], grads_b)]
            row_a.append(first)
            row_b.append(second)
            row_c.append(back_a)
            row_d.append(back_b)
        outs_first.append(jnp.stack(row_a))
        outs_second.append(jnp.stack(row_b))
        back_first.append(jnp.stack(row_c))
        back_second.append(jnp.stack(row_d))
    section_out = jnp.stack([jnp.stack(outs_first), jnp.stack(outs_second)])
    in_grad = jnp.stack([jnp.stack(back_first), jnp.stack(back_second)])
    grads = [jnp.stack([totals[0][k], totals[1][k]]) for k in range(len(weights))]
    return (section_out, in_grad, grads[0], grads[1], grads[2], grads[3], grads[4], grads[5], grads[6], grads[7], grads[8], grads[9], grads[10])
```

```python
import functools

import jax
import jax.numpy as jnp
from jax import lax
from jax.experimental import pallas as pl
from jax.experimental.pallas import tpu as pltpu
from jax.sharding import PartitionSpec as P

EPS = 1e-06
MESH = pl.DeviceIdType.MESH


def snake(pos, side):
    row = pos // side
    col = pos % side
    return row * side + col + (row % 2) * (side - 1 - 2 * col)


def remote(src, dst, send, recv, device):
    return pltpu.make_async_remote_copy(
        src_ref=src,
        dst_ref=dst,
        send_sem=send,
        recv_sem=recv,
        device_id=device,
        device_id_type=MESH,
    )


class Place:
    def __init__(self, ring, line, side):
        self.ring, self.line = ring, line
        self.section = lax.axis_index("section")
        self.ctx = lax.axis_index("ctx")
        self.fsdp = lax.axis_index("fsdp")
        pos = snake(self.ctx, side)
        self.at = lambda step: snake((pos + step + ring) % ring, side)
        self.next = (self.section, self.at(1), self.fsdp)
        self.prev = (self.section, self.at(-1), self.fsdp)

    def peer(self, step):
        return (self.section, self.ctx, (self.fsdp + step) % self.line)

    def greet(self):
        barrier = pltpu.get_barrier_semaphore()
        others = [self.peer(step) for step in range(1, self.line)] + [self.next, self.prev]
        for device in others:
            pl.semaphore_signal(barrier, inc=1, device_id=device, device_id_type=MESH)
        pl.semaphore_wait(barrier, len(others))


def gather_kernel(ring, line, side, count, *refs):
    shards, fulls = refs[:count], refs[count : 2 * count]
    zsend, zrecv, rsend, rrecv, own_sem = refs[2 * count :]
    here = Place(ring, line, side)
    last = ring // 2
    here.greet()

    def bundle(k, ctx):
        return fulls[k].at[pl.ds(ctx * line, line)]

    def half(k, ctx, which):
        return fulls[k].at[pl.ds(ctx * line + which * (line // 2), line // 2)]

    def to_peer(k, step):
        slot = fulls[k].at[here.ctx * line + here.fsdp]
        return remote(shards[k], slot, zsend.at[k, step - 1], zrecv.at[k, step - 1], here.peer(step))

    def hop(k, step, back):
        ctx = here.at(step - 1) if back else here.at(1 - step)
        part = bundle(k, ctx) if step < last else half(k, ctx, back)
        slot = 2 * (step - 1) + back
        return remote(
            part, part, rsend.at[k, slot], rrecv.at[k, slot], here.prev if back else here.next
        )

    started = []

    def begin(copy):
        copy.start()
        started.append(copy)

    own = [
        pltpu.make_async_copy(
            shards[k], fulls[k].at[here.ctx * line + here.fsdp], own_sem.at[k]
        )
        for k in range(count)
    ]
    for k in range(count):
        own[k].start()
        for step in range(1, line):
            begin(to_peer(k, step))
    for tick in range(count + last):
        for step in range(last + 1):
            k = tick - step
            if not 0 <= k < count:
                continue
            if step == 0:
                own[k].wait()
                for other in range(1, line):
                    to_peer(k, other).wait_recv()
            else:
                hop(k, step, 0).wait_recv()
                hop(k, step, 1).wait_recv()
            if step < last:
                begin(hop(k, step + 1, 0))
                begin(hop(k, step + 1, 1))
    for copy in started:
        copy.wait_send()


def gather_weights(shards, ring, line):
    count = len(shards)
    side = int(round(ring**0.5))
    dma = pltpu.SemaphoreType.DMA
    last = ring // 2
    return pl.pallas_call(
        functools.partial(gather_kernel, ring, line, side, count),
        out_shape=[jax.ShapeDtypeStruct((ring * line, *s.shape), s.dtype) for s in shards],
        in_specs=[pl.BlockSpec(memory_space=pltpu.VMEM)] * count,
        out_specs=[pl.BlockSpec(memory_space=pl.ANY)] * count,
        scratch_shapes=[
            dma((count, line - 1)),
            dma((count, line - 1)),
            dma((count, 2 * last)),
            dma((count, 2 * last)),
            dma((count,)),
        ],
        compiler_params=pltpu.CompilerParams(collective_id=0, has_side_effects=True),
    )(*shards)


def reduce_kernel(ring, line, side, count, *refs):
    fulls, shares = refs[:count], refs[count : 2 * count]
    lands = refs[2 * count : 4 * count]
    zlands = refs[4 * count : 5 * count]
    zsend, zrecv, rsend, rrecv = refs[5 * count :]
    here = Place(ring, line, side)
    last = ring // 2
    here.greet()

    def rows(ctx, first, size):
        return pl.ds(ctx * line + first, size)

    def hop(k, step, back):
        ctx = here.at(step - 1 - last) if back else here.at(last - step + 1)
        land = lands[2 * k + back]
        if step == 1:
            first, size = (line // 2 if back else 0), line // 2
        else:
            first, size = 0, line
        return remote(
            fulls[k].at[rows(ctx, first, size)],
            land.at[step - 1, pl.ds(first, size)],
            rsend.at[k, 2 * (step - 1) + back],
            rrecv.at[k, 2 * (step - 1) + back],
            here.prev if back else here.next,
        )

    def absorb(k, step, back):
        ctx = here.at(step - last) if back else here.at(last - step)
        if step == 1:
            first, size = (line // 2 if back else 0), line // 2
        else:
            first, size = 0, line
        at = rows(ctx, first, size)
        mine = fulls[k][at].astype(jnp.float32)
        theirs = lands[2 * k + back][step - 1, pl.ds(first, size)].astype(jnp.float32)
        fulls[k][at] = (mine + theirs).astype(jnp.bfloat16)

    def to_peer(k, step):
        shard = here.ctx * line + (here.fsdp + step) % line
        return remote(
            fulls[k].at[shard],
            zlands[k].at[step - 1],
            zsend.at[k, step - 1],
            zrecv.at[k, step - 1],
            here.peer(step),
        )

    started = []

    def begin(copy):
        copy.start()
        started.append(copy)

    for k in range(count):
        begin(hop(k, 1, 0))
        begin(hop(k, 1, 1))
    for tick in range(count + last):
        for step in range(1, last + 2):
            k = tick - step + 1
            if not 0 <= k < count:
                continue
            if step <= last:
                for back in (0, 1):
                    hop(k, step, back).wait_recv()
                    absorb(k, step, back)
                if step < last:
                    for back in (0, 1):
                        begin(hop(k, step + 1, back))
                else:
                    for other in range(1, line):
                        begin(to_peer(k, other))
            else:
                total = fulls[k][here.ctx * line + here.fsdp].astype(jnp.float32)
                for other in range(1, line):
                    to_peer(k, other).wait_recv()
                    total = total + zlands[k][other - 1].astype(jnp.float32)
                shares[k][...] = total
    for copy in started:
        copy.wait_send()


def reduce_grads(fulls, ring, line):
    count = len(fulls)
    side = int(round(ring**0.5))
    dma = pltpu.SemaphoreType.DMA
    last = ring // 2
    lands = []
    for full in fulls:
        lands += [pltpu.VMEM((last, line, *full.shape[1:]), full.dtype)] * 2
    return pl.pallas_call(
        functools.partial(reduce_kernel, ring, line, side, count),
        out_shape=[jax.ShapeDtypeStruct(full.shape[1:], jnp.float32) for full in fulls],
        in_specs=[pl.BlockSpec(memory_space=pltpu.VMEM)] * count,
        out_specs=[pl.BlockSpec(memory_space=pltpu.VMEM)] * count,
        scratch_shapes=lands
        + [pltpu.VMEM((line - 1, *full.shape[1:]), full.dtype) for full in fulls]
        + [
            dma((count, line - 1)),
            dma((count, line - 1)),
            dma((count, 2 * last)),
            dma((count, 2 * last)),
        ],
        compiler_params=pltpu.CompilerParams(
            collective_id=1, has_side_effects=True, vmem_limit_bytes=58 << 20
        ),
    )(*fulls)


def pack_gains(gains, rows):
    columns = [jnp.pad(g, (0, rows - g.shape[0])) for g in gains]
    return jnp.pad(jnp.stack(columns, axis=1), ((0, 0), (0, 128 - len(gains))))


def gather_all(shards):
    ring, line = lax.axis_size("ctx"), lax.axis_size("fsdp")
    wq, wk, wv, wo, wg, wu, wd, *gains = [shard[0] for shard in shards]
    rows = wq.shape[0]
    packed = [
        jnp.concatenate([wq, wk, wv, pack_gains(gains, rows)], axis=1),
        wo,
        wg,
        wu,
        wd,
    ]
    qkv, wo, wg, wu, wd = gather_weights(packed, ring, line)
    cuts = [wq.shape[1], wq.shape[1] + wk.shape[1], wq.shape[1] + 2 * wk.shape[1]]
    flat = lambda full: full.reshape(-1, full.shape[-1])
    full = flat(qkv)
    gain_block = qkv[:, :, cuts[2] :]
    return (
        full[:, : cuts[0]],
        full[:, cuts[0] : cuts[1]],
        full[:, cuts[1] : cuts[2]],
        flat(wo),
        flat(wg),
        flat(wu),
        flat(wd),
        *[gain_block[:, : g.shape[0], i].reshape(-1) for i, g in enumerate(gains)],
    )


def reduce_all(grads, shards):
    ring, line = lax.axis_size("ctx"), lax.axis_size("fsdp")
    count = ring * line
    gq, gk, gv, go, gg, gu, gd, *gains = grads
    gain_parts = [g.reshape(count, -1) for g in gains]
    rows = gq.shape[0] // count
    columns = [jnp.pad(g, ((0, 0), (0, rows - g.shape[1]))) for g in gain_parts]
    block = jnp.pad(jnp.stack(columns, axis=2), ((0, 0), (0, 0), (0, 128 - len(gains))))
    split = lambda g: g.reshape(count, -1, g.shape[-1])
    qkv = jnp.concatenate([split(gq), split(gk), split(gv), block], axis=2)
    packed = [part.astype(jnp.bfloat16) for part in (split(gd), split(gg), split(gu), split(go), qkv)]
    gd, gg, gu, go, qkv = reduce_grads(packed, ring, line)
    cuts = [gq.shape[1], gq.shape[1] + gk.shape[1], gq.shape[1] + 2 * gk.shape[1]]
    block = qkv[:, cuts[2] :]
    parts = [qkv[:, : cuts[0]], qkv[:, cuts[0] : cuts[1]], qkv[:, cuts[1] : cuts[2]], go, gg, gu, gd]
    parts += [block[: g.shape[1], i] for i, g in enumerate(gain_parts)]
    return tuple(part[None] for part in parts)


def shifted(shard, axis, by):
    count = lax.axis_size(axis)
    pairs = [(i, i + by) for i in range(count) if 0 <= i + by < count]
    return lax.ppermute(shard, axis, pairs)


def rms_scale(values, gain):
    mean_square = jnp.mean(values * values, axis=-1, keepdims=True)
    return values * lax.rsqrt(mean_square + EPS) * gain


def norm_pull(values, gain, upstream):
    _, pull = jax.vjp(rms_scale, values, gain)
    return pull(upstream)


def glu_act(gate_part, up_part):
    return jax.nn.gelu(gate_part, approximate=True) * up_part


def fdot(left, right):
    return jnp.dot(left, right, preferred_element_type=jnp.float32)


def fsum(form, left, right):
    return jnp.einsum(form, left, right, preferred_element_type=jnp.float32)


def masked_scores(query_n, key_n, query_pos, key_pos):
    head_dim = query_n.shape[-1]
    scores = fsum("rhd,sd->hrs", query_n, key_n) * head_dim ** (-0.5)
    allowed = key_pos[None, None, :] <= query_pos[None, :, None]
    return jnp.where(allowed, scores, -jnp.inf)


def layer_forward(inputs, params, query_pos, key_pos):
    w_query, w_key, w_value, w_out, w_gate, w_up, w_down, g_attn, g_ffn, g_query, g_key = params
    head_dim = g_query.shape[0]
    count = inputs.shape[0]
    resid = inputs.astype(jnp.float32)
    normed = rms_scale(resid, g_attn.astype(jnp.float32)).astype(jnp.bfloat16)
    query = fdot(normed, w_query)
    key_raw = fdot(normed, w_key)
    value = fdot(normed, w_value).astype(jnp.bfloat16)
    query_n = rms_scale(query.reshape(count, -1, head_dim), g_query.astype(jnp.float32)).astype(
        jnp.bfloat16
    )
    key_n = rms_scale(key_raw, g_key.astype(jnp.float32)).astype(jnp.bfloat16)
    local_kv = jnp.concatenate([key_n, value], axis=1)
    keyval = lax.all_gather(local_kv, "ctx", axis=0, tiled=True)
    scores = masked_scores(query_n, keyval[:, :head_dim], query_pos, key_pos)
    top = jnp.max(scores, axis=-1, keepdims=True)
    lse = top + jnp.log(jnp.sum(jnp.exp(scores - top), axis=-1, keepdims=True))
    probs = jnp.exp(scores - lse).astype(jnp.bfloat16)
    mixed = fsum("hrs,sd->rhd", probs, keyval[:, head_dim:]).reshape(count, -1).astype(jnp.bfloat16)
    middle = resid + fdot(mixed, w_out)
    ffn_in = rms_scale(middle, g_ffn.astype(jnp.float32)).astype(jnp.bfloat16)
    hidden = glu_act(fdot(ffn_in, w_gate), fdot(ffn_in, w_up)).astype(jnp.bfloat16)
    result = middle + fdot(hidden, w_down)
    return (result.astype(jnp.bfloat16), (inputs, query, key_raw, keyval, lse, mixed, middle))


def layer_backward(saved, upstream, params, query_pos, key_pos):
    w_query, w_key, w_value, w_out, w_gate, w_up, w_down, g_attn, g_ffn, g_query, g_key = params
    inputs, query, key_raw, keyval, lse, mixed, middle = saved
    head_dim = g_query.shape[0]
    count = inputs.shape[0]
    gain_a = g_attn.astype(jnp.float32)
    gain_f = g_ffn.astype(jnp.float32)
    gain_q = g_query.astype(jnp.float32)
    gain_k = g_key.astype(jnp.float32)
    resid = inputs.astype(jnp.float32)
    ffn_in = rms_scale(middle, gain_f).astype(jnp.bfloat16)
    gate_part = fdot(ffn_in, w_gate)
    up_part = fdot(ffn_in, w_up)
    hidden = glu_act(gate_part, up_part).astype(jnp.bfloat16)
    top_b = upstream.astype(jnp.bfloat16)
    grad_down = fsum("rf,rd->fd", hidden, top_b)
    dhidden = fsum("rd,fd->rf", top_b, w_down)
    _, pull = jax.vjp(glu_act, gate_part, up_part)
    dgate, dup = pull(dhidden)
    dgate_b = dgate.astype(jnp.bfloat16)
    dup_b = dup.astype(jnp.bfloat16)
    grad_gate = fsum("rd,rf->df", ffn_in, dgate_b)
    grad_up = fsum("rd,rf->df", ffn_in, dup_b)
    dffn = fsum("rf,df->rd", dgate_b, w_gate) + fsum("rf,df->rd", dup_b, w_up)
    dmid_norm, grad_gf = norm_pull(middle, gain_f, dffn)
    dmiddle = upstream + dmid_norm
    dmid_b = dmiddle.astype(jnp.bfloat16)
    grad_out = fsum("rk,rd->kd", mixed, dmid_b)
    dmixed = fsum("rd,kd->rk", dmid_b, w_out).astype(jnp.bfloat16)
    query_heads = query.reshape(count, -1, head_dim)
    query_n = rms_scale(query_heads, gain_q).astype(jnp.bfloat16)
    key_n = keyval[:, :head_dim]
    value = keyval[:, head_dim:]
    scores = masked_scores(query_n, key_n, query_pos, key_pos)
    probs = jnp.exp(scores - lse)
    dout = dmixed.reshape(count, -1, head_dim)
    dvalue = fsum("hrs,rhd->sd", probs.astype(jnp.bfloat16), dout)
    dprobs = fsum("rhd,sd->hrs", dout, value)
    inner = jnp.sum(probs * dprobs, axis=-1, keepdims=True)
    dscore = (probs * (dprobs - inner) * head_dim ** (-0.5)).astype(jnp.bfloat16)
    dquery_n = fsum("hrs,sd->rhd", dscore, key_n)
    dkey_n = fsum("hrs,rhd->sd", dscore, query_n)
    dkv_full = jnp.concatenate([dkey_n, dvalue], axis=1)
    dkv = lax.psum_scatter(
        dkv_full.astype(jnp.bfloat16), "ctx", scatter_dimension=0, tiled=True
    ).astype(jnp.float32)
    dquery, grad_gq = norm_pull(query_heads, gain_q, dquery_n)
    dkey, grad_gk = norm_pull(key_raw, gain_k, dkv[:, :head_dim])
    dq_b = dquery.reshape(count, -1).astype(jnp.bfloat16)
    dk_b = dkey.astype(jnp.bfloat16)
    dv_b = dkv[:, head_dim:].astype(jnp.bfloat16)
    normed = rms_scale(resid, gain_a).astype(jnp.bfloat16)
    grad_q = fsum("rd,rk->dk", normed, dq_b)
    grad_k = fsum("rd,rk->dk", normed, dk_b)
    grad_v = fsum("rd,rk->dk", normed, dv_b)
    dnormed = (
        fsum("rk,dk->rd", dq_b, w_query)
        + fsum("rk,dk->rd", dk_b, w_key)
        + fsum("rk,dk->rd", dv_b, w_value)
    )
    dres_norm, grad_ga = norm_pull(resid, gain_a, dnormed)
    dinput = dmiddle + dres_norm
    grads = (
        grad_q,
        grad_k,
        grad_v,
        grad_out,
        grad_gate,
        grad_up,
        grad_down,
        grad_ga,
        grad_gf,
        grad_gq,
        grad_gk,
    )
    return (dinput.astype(jnp.bfloat16), grads)


def body(
    tokens,
    cotangent,
    block_map,
    order,
    w_query,
    w_key,
    w_value,
    w_out,
    w_gate,
    w_up,
    w_down,
    g_attn,
    g_ffn,
    g_query,
    g_key,
):
    micro = tokens.shape[0]
    seq_rows = tokens.shape[2]
    width = tokens.shape[3]
    half = seq_rows // 2
    section = lax.axis_index("section")
    ctx_index = lax.axis_index("ctx")
    starts = block_map.reshape(-1) * half
    key_pos = (starts[:, None] + jnp.arange(half, dtype=jnp.int32)[None, :]).reshape(-1)
    query_pos = lax.dynamic_slice_in_dim(key_pos, ctx_index * seq_rows, seq_rows)
    shards = (w_query, w_key, w_value, w_out, w_gate, w_up, w_down, g_attn, g_ffn, g_query, g_key)
    params = gather_all(shards)
    received = jnp.zeros((seq_rows, width), jnp.bfloat16)
    outputs = []
    saved_list = []
    for forward_tick in range(micro + 1):
        picked = order[0, min(forward_tick, micro - 1)]
        chosen = lax.dynamic_index_in_dim(tokens[:, 0], picked, 0, keepdims=False)
        inputs = jnp.where(section == 0, chosen, received)
        result, saved = layer_forward(inputs, params, query_pos, key_pos)
        outputs.append(result)
        saved_list.append(saved)
        if forward_tick < micro:
            received = shifted(result, "section", 1)
    stacked = jax.tree.map(lambda *parts: jnp.stack(parts), *saved_list)
    section_out = lax.dynamic_slice_in_dim(jnp.stack(outputs), section, micro, 0)
    totals = (0.0,) * len(shards)
    back_received = jnp.zeros((seq_rows, width), jnp.bfloat16)
    grads_in = []
    for backward_tick in range(micro + 1):
        slot_index = backward_tick - 1 + section
        valid = ((slot_index >= 0) & (slot_index < micro)).astype(jnp.float32)
        saved_at = jnp.clip(backward_tick - 1 + 2 * section, 0, micro)
        saved = jax.tree.map(
            lambda stack_part: lax.dynamic_index_in_dim(stack_part, saved_at, 0, keepdims=False),
            stacked,
        )
        arriving = jnp.where(
            section == 1, cotangent[min(backward_tick, micro - 1), 0], back_received
        )
        upstream = arriving.astype(jnp.float32) * valid
        dinput, grads = layer_backward(saved, upstream, params, query_pos, key_pos)
        grads_in.append(dinput)
        if backward_tick < micro:
            back_received = shifted(dinput, "section", -1)
        totals = tuple((acc + grad for acc, grad in zip(totals, grads)))
    totals = reduce_all(totals, shards)
    in_grad = lax.dynamic_slice_in_dim(jnp.stack(grads_in), 1 - section, micro, 0)
    section_out = section_out.reshape(1, micro, 1, seq_rows, width)
    in_grad = in_grad.reshape(1, micro, 1, seq_rows, width)
    return (
        section_out,
        in_grad,
        totals[0],
        totals[1],
        totals[2],
        totals[3],
        totals[4],
        totals[5],
        totals[6],
        totals[7],
        totals[8],
        totals[9],
        totals[10],
    )


def solution(mesh):
    in_specs = (
        P(None, "fsdp", "ctx", None),
        P(None, "fsdp", "ctx", None),
        P(),
        P("fsdp", None),
        P("section", ("ctx", "fsdp"), None),
        P("section", ("ctx", "fsdp"), None),
        P("section", ("ctx", "fsdp"), None),
        P("section", ("ctx", "fsdp"), None),
        P("section", ("ctx", "fsdp"), None),
        P("section", ("ctx", "fsdp"), None),
        P("section", ("ctx", "fsdp"), None),
        P("section", ("ctx", "fsdp")),
        P("section", ("ctx", "fsdp")),
        P("section", ("ctx", "fsdp")),
        P("section", ("ctx", "fsdp")),
    )
    out_specs = (
        P("section", None, "fsdp", "ctx", None),
        P("section", None, "fsdp", "ctx", None),
        P("section", ("ctx", "fsdp"), None),
        P("section", ("ctx", "fsdp"), None),
        P("section", ("ctx", "fsdp"), None),
        P("section", ("ctx", "fsdp"), None),
        P("section", ("ctx", "fsdp"), None),
        P("section", ("ctx", "fsdp"), None),
        P("section", ("ctx", "fsdp"), None),
        P("section", ("ctx", "fsdp")),
        P("section", ("ctx", "fsdp")),
        P("section", ("ctx", "fsdp")),
        P("section", ("ctx", "fsdp")),
    )
    return jax.shard_map(body, mesh=mesh, in_specs=in_specs, out_specs=out_specs, check_vma=False)
```
